32 devices in a mesh: occ: 2 (over x), vir: 4 (over z), aux: 4 (over y, core).
Axes of the slice: x: 2, y: 2, z: 4, core: 2. Of those that a mesh axis runs over, the one named last changes fastest.
Arguments:
- amplitudes: bfloat16 [16, 1024, 1024], P('occ', 'vir'), may hold values from -6 to 6
- pair_mask: int32 [16, 8, 8], P('occ', 'vir'), may hold values 0 or 1
- left_factor: bfloat16 [32, 1024, 4096], P(None, 'vir', 'aux'), may hold values from -0.0390625 to 0.0390625
- left_mask: int32 [8, 32], P('vir', 'aux'), may hold values 0 or 1
- right_factor: bfloat16 [1024, 4, 4096], P(('occ', 'vir'), None, 'aux'), may hold values from -0.0390625 to 0.0390625
- right_mask: int32 [8, 32], P(None, 'aux'), may hold values 0 or 1
- residual_in: float32 [16, 4, 32], P('occ'), may hold values from -6 to 6
Outputs:
- updated: float32 [16, 4, 32], P('occ')
The draws below stay inside these ranges and needn't reach their ends.
All inputs are finite; a program needn't handle non-finite values. No bound on the sum of `pair_mask` or of `left_mask` or of `right_mask` on one device may be relied on, other than what follows from the above.
Results may differ from the reference program's by a relative error of at most 0.0003.
Values may be sent and summed in bfloat16 or wider, within the bound.
A program may use at most 128 MiB of HBM per device.

```python
import jax
import jax.numpy as jnp
from jax import lax

V = 1024
NAUX = 4096
TILE = 128
AW = 32
BW = 4
PAIRS = 16
NVT = 8
NQT = 32


def set_ends(entries, own_key, smallest, top_value):
    dims = entries.shape
    place = [jax.random.randint(jax.random.fold_in(own_key, axis), (), 0, dims[axis]) for axis in range(len(dims))]
    entries = entries.at[tuple(place)].set(smallest)
    longest = dims.index(max(dims))
    place[longest] = (place[longest] + 1) % dims[longest]
    return entries.at[tuple(place)].set(top_value)


def block_levels(rng, dims, cuts, low, high):
    def one(dim, parts):
        draws = jax.random.uniform(jax.random.fold_in(jax.random.fold_in(rng, 6), dim), (parts,), jnp.float32, low / len(cuts), high / len(cuts))
        return jnp.repeat(jnp.exp(draws), dims[dim] // parts).reshape((-1,) + (1,) * (len(dims) - dim - 1))

    level = one(*cuts[0])
    for cut in cuts[1:]:
        level = level * one(*cut)
    return level


def scatter_about(rng, shape, spread, bound, split=(), kind=jnp.bfloat16):
    drawn = spread * jax.random.normal(rng, shape, jnp.float32)
    if split:
        drawn = drawn * block_levels(rng, shape, split, -0.22, 0.18)
    return jnp.clip(drawn, -bound, bound).astype(kind)


def setup_inputs(seed: int = 0) -> dict:
    key_list = jax.random.split(jax.random.key(seed), 8)
    return {
        "amplitudes": scatter_about(key_list[0], (PAIRS, V, V), 1.0, 6.0, ((0, 2), (1, 4))),
        "pair_mask": set_ends((jax.random.randint(key_list[1], (PAIRS, NVT, NVT), 0, 4) < 3).astype(jnp.int32), jax.random.fold_in(key_list[1], 1), 0, 1),
        "left_factor": scatter_about(key_list[2], (AW, V, NAUX), (V * max(2, NAUX // 150)) ** -0.5, 0.0390625, ((1, 4), (2, 4))),
        "left_mask": set_ends((jax.random.randint(key_list[3], (NVT, NQT), 0, 2) < 1).astype(jnp.int32), jax.random.fold_in(key_list[3], 1), 0, 1),
        "right_factor": scatter_about(key_list[4], (V, BW, NAUX), (V * max(2, NAUX // 150)) ** -0.5, 0.0390625, ((0, 8), (2, 4))),
        "right_mask": set_ends((jax.random.randint(key_list[5], (NVT, NQT), 0, 2) < 1).astype(jnp.int32), jax.random.fold_in(key_list[5], 1), 0, 1),
        "residual_in": scatter_about(key_list[6], (PAIRS, BW, AW), 1.0, 6.0, ((0, 2),), jnp.float32),
    }


def expand_tiles(mask, width):
    grown = jnp.repeat(jnp.repeat(mask, width, axis=-2), width, axis=-1)
    return grown.astype(jnp.float32)


def reference(amplitudes, pair_mask, left_factor, left_mask, right_factor, right_mask, residual_in):
    left = left_factor.astype(jnp.float32) * expand_tiles(left_mask, TILE)[None, :, :]
    right = right_factor.astype(jnp.float32) * expand_tiles(right_mask, TILE)[:, None, :]
    right_flat = right.reshape(V, BW * NAUX)

    def one_pair(pieces):
        amp, msk = pieces
        tau = amp.astype(jnp.float32) * expand_tiles(msk, TILE)
        inner = jnp.dot(tau, right_flat, precision=lax.Precision.HIGHEST, preferred_element_type=jnp.float32)
        inner = inner.reshape(V, BW, NAUX)
        return jnp.einsum("cbq,acq->ba", inner, left, precision=lax.Precision.HIGHEST)

    ladder = lax.map(one_pair, (amplitudes, pair_mask))
    return residual_in + ladder
```

```python
import functools

import jax
import jax.numpy as jnp
from jax import lax
from jax.experimental import pallas as pl
from jax.experimental.pallas import tpu as pltpu
from jax.sharding import PartitionSpec as P

TILE = 128
QC = 256
CC = 32
MESH = pl.DeviceIdType.MESH
F32 = jnp.float32
BF16 = jnp.bfloat16


def kernel(
    no, nv, na, pair_mask, left_mask, right_mask, amp_hbm, left_hbm, right_hbm, res,
    out, amp, left, rbuf, wr, tau, tsend, lhs2, rhs2, acc, part, parts,
    amp_sem, left_sem, own_sem, r_send, r_recv, t_send, t_recv, a_send, a_recv,
):
    occ, vir, aux = lax.axis_index("occ"), lax.axis_index("vir"), lax.axis_index("aux")
    pairs, cols, virt = amp.shape
    nq, _, bq = right_hbm.shape
    rows = rbuf.shape[2]
    block_b = bq // QC
    block_a = left.shape[0]
    cq, depth = tau.shape[3], tau.shape[4]
    pall = no * pairs
    steps = cols // CC
    subs = cq // CC
    groups = CC // 8

    def right_copy(u, n, down, own):
        src = right_hbm.at[n] if own else rbuf.at[u, n]
        return pltpu.make_async_remote_copy(
            src_ref=src,
            dst_ref=rbuf.at[u, n],
            send_sem=r_send.at[1 if down else 0, u, n],
            recv_sem=r_recv.at[u, n],
            device_id={"vir": vir - 1 if down else vir + 1},
            device_id_type=MESH,
        )

    def send_own(n):
        @pl.when(vir > 0)
        def _():
            right_copy(vir, n, True, True).start()

        @pl.when(vir < nv - 1)
        def _():
            right_copy(vir, n, False, True).start()

    def arrive(k, n, forwarded):
        for down in (True, False):
            u = vir + k if down else vir - k
            here = u < nv if down else u >= 0
            passes = vir > 0 if down else vir < nv - 1

            @pl.when(here & (passes if forwarded else jnp.logical_not(passes)))
            def _():
                right_copy(u, n, down, False).wait_recv()
                if forwarded:
                    right_copy(u, n, down, False).start()

    amp_copy = pltpu.make_async_copy(amp_hbm, amp, amp_sem)
    amp_copy.start()
    send_own(0)
    if nq > 1:
        send_own(1)
    own_copies = [
        pltpu.make_async_copy(right_hbm.at[n], rbuf.at[vir, n], own_sem.at[n]) for n in range(nq)
    ]
    for copy in own_copies:
        copy.start()

    def left_copy(n):
        return pltpu.make_async_copy(
            left_hbm.at[:, :, pl.ds(pl.multiple_of(n * QC, QC), QC)],
            left.at[:, :, pl.ds(pl.multiple_of(n * QC, QC), QC)],
            left_sem.at[n],
        )

    for n in range(nq):
        left_copy(n).start()
    amp_copy.wait()

    piece = min(cq, TILE)

    def masked(p, row, column):
        m = pair_mask[p, row // TILE, column // TILE].astype(F32)
        block = amp[
            p, pl.ds(pl.multiple_of(row, piece), piece), pl.ds(pl.multiple_of(column, TILE), TILE)
        ]
        return (block.astype(F32) * m).astype(BF16)

    def fill_send(p, carry):
        for k in range(1, no):
            base = lax.rem(occ + k, no) * depth
            for off in range(0, cq, piece):
                for col in range(0, depth, TILE):
                    tsend[k - 1, p, off : off + piece, col : col + TILE] = masked(
                        p, aux * cq + off, base + col
                    )
        return carry

    lax.fori_loop(0, pairs, fill_send, 0)

    def tau_copy(k, sem, q, src, device):
        slot = lax.rem(occ + k, no)
        return pltpu.make_async_remote_copy(
            src_ref=src,
            dst_ref=tau.at[slot, q],
            send_sem=t_send.at[k, sem],
            recv_sem=t_recv.at[slot, q],
            device_id=device,
            device_id_type=MESH,
        )

    def occ_copy(k):
        return pltpu.make_async_remote_copy(
            src_ref=tsend.at[k - 1],
            dst_ref=tau.at[occ, aux],
            send_sem=t_send.at[k, 0],
            recv_sem=t_recv.at[occ, aux],
            device_id={"occ": lax.rem(occ + k, no)},
            device_id_type=MESH,
        )

    acc[...] = jnp.zeros_like(acc)
    for k in range(1, no):
        occ_copy(k).start()

    def fill_own(i, carry):
        p, q = i // na, lax.rem(i, na)
        for off in range(0, cq, piece):
            for col in range(0, depth, TILE):
                tau[occ, q, p, off : off + piece, col : col + TILE] = masked(
                    p, q * cq + off, occ * depth + col
                )
        return carry

    lax.fori_loop(0, pairs * na, fill_own, 0)

    bits = []
    bit = na // 2
    while bit:
        bits.append(bit)
        bit //= 2
    have = [0]
    sent = 1
    tau_sends = [occ_copy(k) for k in range(1, no)]
    waves = list(range(1, nv))
    arrive(1, 0, True)
    for stage, bit in enumerate(bits):
        for k in range(1, no):
            for m in have if stage == 0 else have[len(have) // 2 :]:
                q = aux ^ m
                tau_copy(k, 0, q, tau.at[lax.rem(occ + k, no), q], {"aux": aux ^ bit}).wait_recv()
            for i, m in enumerate(have):
                q = aux ^ m
                copy = tau_copy(
                    k, sent + i, q, tau.at[lax.rem(occ + k, no), q], {"aux": aux ^ bit}
                )
                copy.start()
                tau_sends.append(copy)
        sent += len(have)
        have = have + [m ^ bit for m in have]
        if stage == 0:
            for k in waves[1:]:
                arrive(k, 0, True)
            if nq > 2:
                send_own(2)
    for k in range(1, no):
        for m in have[len(have) // 2 :] if bits else have:
            q = aux ^ m
            tau_copy(k, 0, q, tau.at[lax.rem(occ + k, no), q], {"occ": lax.rem(occ + k, no)}).wait_recv()
    for copy in own_copies:
        copy.wait()

    sub_rows = min(rows, TILE)
    lane = lax.broadcasted_iota(jnp.int32, (1, QC), 1)

    def step(it, carry):
        n = it // steps
        cs = lax.rem(it, steps)

        @pl.when(cs == 0)
        def _():
            for k in waves:
                arrive(k, n, False)
            left_copy(n).wait()
            for u in range(nv):
                for r in range(0, rows, sub_rows):
                    dt = (occ * depth + u * rows + r) // TILE
                    m = jnp.zeros((1, QC), F32)
                    for t in range(QC // TILE):
                        m = jnp.where(
                            lane // TILE == t, right_mask[dt, n * (QC // TILE) + t].astype(F32), m
                        )
                    for b in range(block_b):
                        x = rbuf[u, n, pl.ds(r, sub_rows), b * QC : (b + 1) * QC]
                        wr[u * rows + r : u * rows + r + sub_rows, b * QC : (b + 1) * QC] = (
                            x.astype(F32) * m
                        ).astype(BF16)

        for k in waves:
            @pl.when((cs == min(2 * k, steps - 1)) & (n + 1 < nq))
            def _():
                arrive(k, n + 1, True)
                if k == nv - 1:
                    @pl.when(n + 3 < nq)
                    def _():
                        send_own(n + 3)

        c0 = pl.multiple_of(cs * CC, CC)
        q0 = pl.multiple_of(n * QC, QC)
        lm = jnp.zeros((1, QC), F32)
        for t in range(QC // TILE):
            lm = jnp.where(
                lane // TILE == t, left_mask[cs * CC // TILE, n * (QC // TILE) + t].astype(F32), lm
            )
        w = left[:, pl.ds(c0, CC), pl.ds(q0, QC)].astype(F32) * lm[None]
        w = w.reshape(block_a, groups, 8, QC)
        for j in range(groups):
            rhs2[:, j * QC : (j + 1) * QC] = w[:, j].reshape(block_a * 8, QC).astype(BF16)
        q, s = cs // subs, lax.rem(cs, subs)
        t = tau[:, q, :, pl.ds(pl.multiple_of(s * CC, CC), CC), :].reshape(pall * CC, depth)
        half = pall * 8
        for b in range(block_b):
            inner = jnp.dot(t, wr[:, b * QC : (b + 1) * QC], preferred_element_type=F32)
            inner = inner.reshape(pall, groups, 8, QC)
            for j in range(groups):
                x = inner[:, j].reshape(half, QC)
                hi = x.astype(BF16)
                lo = (x - hi.astype(F32)).astype(BF16)
                lhs2[2 * b * half : (2 * b + 1) * half, j * QC : (j + 1) * QC] = hi
                lhs2[(2 * b + 1) * half : (2 * b + 2) * half, j * QC : (j + 1) * QC] = lo
            sl = slice(2 * b * half, (2 * b + 2) * half)
            acc[sl, :] += lax.dot_general(
                lhs2[sl, :], rhs2[...], (((1,), (1,)), ((), ())), preferred_element_type=F32
            )
        return carry

    lax.fori_loop(0, nq * steps, step, 0)

    half = pall * 8
    width = block_a * 8
    row_i = lax.rem(lax.broadcasted_iota(jnp.int32, (half, width), 0), 8)
    col_i = lax.rem(lax.broadcasted_iota(jnp.int32, (half, width), 1), 8)
    diag = (row_i == col_i).astype(F32)
    total = jnp.zeros((pall, block_b * block_a), F32)
    src = lax.broadcasted_iota(jnp.int32, (width, block_b * block_a), 0) // 8
    dst = lax.broadcasted_iota(jnp.int32, (width, block_b * block_a), 1)
    for b in range(block_b):
        y = acc[2 * b * half : (2 * b + 1) * half, :] + acc[(2 * b + 1) * half : (2 * b + 2) * half, :]
        y = (y * diag).reshape(pall, 8, width).sum(axis=1)
        pick = (src + b * block_a == dst).astype(F32)
        total += jnp.dot(y, pick, precision=lax.Precision.HIGHEST, preferred_element_type=F32)
    part[...] = total.reshape(no, pairs, block_b * block_a)

    devices = no * nv * na
    me = (occ * nv + vir) * na + aux
    parts[me] = part[occ]

    def final_copy(k):
        j = lax.rem(me + k, devices)
        to = (j // (nv * na), lax.rem(j // na, nv), lax.rem(j, na))
        return pltpu.make_async_remote_copy(
            src_ref=part.at[to[0]],
            dst_ref=parts.at[me],
            send_sem=a_send.at[k],
            recv_sem=a_recv.at[me],
            device_id=to,
            device_id_type=MESH,
        )

    def final_arrival(k):
        j = lax.rem(me + k, devices)
        to = (j // (nv * na), lax.rem(j // na, nv), lax.rem(j, na))
        return pltpu.make_async_remote_copy(
            src_ref=part.at[to[0]],
            dst_ref=parts.at[j],
            send_sem=a_send.at[k],
            recv_sem=a_recv.at[j],
            device_id=to,
            device_id_type=MESH,
        )

    def start_final(k, carry):
        final_copy(k).start()
        return carry

    def wait_final(k, carry):
        final_arrival(k).wait_recv()
        return carry

    def drain_final(k, carry):
        final_copy(k).wait_send()
        return carry

    lax.fori_loop(1, devices, start_final, 0)
    for copy in tau_sends:
        copy.wait_send()
    for n in range(nq):
        for down in (True, False):
            passes = vir > 0 if down else vir < nv - 1

            @pl.when(passes)
            def _():
                right_copy(vir, n, down, True).wait_send()

            for k in waves:
                u = vir + k if down else vir - k
                here = u < nv if down else u >= 0

                @pl.when(passes & here)
                def _():
                    right_copy(u, n, down, False).wait_send()
    lax.fori_loop(1, devices, wait_final, 0)
    out[...] = res[...] + jnp.sum(parts[...], axis=0)
    lax.fori_loop(1, devices, drain_final, 0)


def local(sizes, amplitudes, pair_mask, left_factor, left_mask, right_factor, right_mask, residual_in):
    no, nv, na = sizes
    pairs, cols, virt = amplitudes.shape
    rows, block_b, auxn = right_factor.shape
    block_a = left_factor.shape[0]
    nq = auxn // QC
    depth = rows * nv
    cq = cols // na
    pall = no * pairs
    right = right_factor.reshape(rows, block_b, nq, QC).transpose(2, 0, 1, 3)
    right = right.reshape(nq, rows, block_b * QC)
    ba = block_b * block_a
    vmem = pl.BlockSpec(memory_space=pltpu.VMEM)
    smem = pl.BlockSpec(memory_space=pltpu.SMEM)
    hbm = pl.BlockSpec(memory_space=pltpu.MemorySpace.HBM)
    dma = pltpu.SemaphoreType.DMA
    out = pl.pallas_call(
        functools.partial(kernel, no, nv, na),
        out_shape=jax.ShapeDtypeStruct((pairs, ba), F32),
        in_specs=[smem, smem, smem, hbm, hbm, hbm, vmem],
        out_specs=vmem,
        scratch_shapes=[
            pltpu.VMEM((pairs, cols, virt), BF16),
            pltpu.VMEM(left_factor.shape, BF16),
            pltpu.VMEM((nv, nq, rows, block_b * QC), BF16),
            pltpu.VMEM((depth, block_b * QC), BF16),
            pltpu.VMEM((no, na, pairs, cq, depth), BF16),
            pltpu.VMEM((max(no - 1, 1), pairs, cq, depth), BF16),
            pltpu.VMEM((2 * block_b * pall * 8, CC // 8 * QC), BF16),
            pltpu.VMEM((block_a * 8, CC // 8 * QC), BF16),
            pltpu.VMEM((2 * block_b * pall * 8, block_a * 8), F32),
            pltpu.VMEM((no, pairs, ba), F32),
            pltpu.VMEM((no * nv * na, pairs, ba), F32),
            dma,
            dma((nq,)),
            dma((nq,)),
            dma((2, nv, nq)),
            dma((nv, nq)),
            dma((no, na)),
            dma((no, na)),
            dma((no * nv * na,)),
            dma((no * nv * na,)),
        ],
        compiler_params=pltpu.CompilerParams(
            has_side_effects=True, vmem_limit_bytes=62 * 1024 * 1024
        ),
        name="ladder",
    )(pair_mask, left_mask, right_mask, amplitudes, left_factor, right,
      residual_in.reshape(pairs, ba))
    return out.reshape(pairs, block_b, block_a)


def solution(mesh):
    sizes = tuple(mesh.shape[name] for name in ("occ", "vir", "aux"))
    return jax.shard_map(
        functools.partial(local, sizes),
        mesh=mesh,
        in_specs=(
            P("occ", "vir", None),
            P("occ", "vir", None),
            P(None, "vir", "aux"),
            P("vir", "aux"),
            P(("occ", "vir"), None, "aux"),
            P(None, "aux"),
            P("occ", None, None),
        ),
        out_specs=P("occ", None, None),
        check_vma=False,
    )
```
